32 devices in a mesh: pair: 1 (over z), tp: 4 (over y), node: 8 (over x, core).
Axes of the slice: x: 4, y: 4, z: 1, core: 2. Of those that a mesh axis runs over, the one named last changes fastest.
The devices are a block of a 4x4x8 slice.
Arguments:
- prompt: bfloat16 [8, 2048, 4096], P(('pair', 'node'))
- s_len: int32 [8], P(('pair', 'node'))
- tokens: bfloat16 [8, 16, 4096], P(('pair', 'node'))
- c_len: int32 [8, 16], P(('pair', 'node'))
- k_cache: bfloat16 [1, 8, 16, 512, 8, 128], P(None, ('pair', 'node'), None, None, 'tp')
- v_cache: bfloat16 [1, 8, 16, 512, 8, 128], P(None, ('pair', 'node'), None, None, 'tp')
- attn_norm: bfloat16 [1, 4096], replicated
- mlp_norm: bfloat16 [1, 4096], replicated
- w_qkv_pre: bfloat16 [1, 4096, 8, 6, 128], P(None, None, 'tp')
- w_out_pre: bfloat16 [1, 8, 4, 128, 4096], P(None, 'tp')
- w_qkv_dec: bfloat16 [1, 4096, 8, 6, 128], P(None, None, 'tp')
- w_out_dec: bfloat16 [1, 8, 4, 128, 4096], P(None, 'tp')
- w_gate: bfloat16 [1, 4096, 14336], P(None, None, 'tp')
- w_up: bfloat16 [1, 4096, 14336], P(None, None, 'tp')
- w_down: bfloat16 [1, 14336, 4096], P(None, 'tp')
Outputs:
- output 1: bfloat16 [8, 2048, 4096], P(('pair', 'node'))
- output 2: bfloat16 [8, 16, 4096], P(('pair', 'node'))
- output 3: bfloat16 [1, 8, 2048, 8, 128], P(None, ('pair', 'node'), None, 'tp')
- output 4: bfloat16 [1, 8, 2048, 8, 128], P(None, ('pair', 'node'), None, 'tp')
- output 5: bfloat16 [1, 8, 16, 512, 8, 128], P(None, ('pair', 'node'), None, None, 'tp')
- output 6: bfloat16 [1, 8, 16, 512, 8, 128], P(None, ('pair', 'node'), None, None, 'tp')
All inputs are finite; a program needn't handle non-finite values.
Results may differ from the reference program's by a relative error of at most 0.00940803.
Values are sent between devices in bfloat16 or wider.
A program may use at most 768 MiB of HBM per device.

```python
import math
import jax
import jax.numpy as jnp
from jax import lax

NODE = 8
TP = 4
S = 2048
BD = 16
T = 512
L = 1
D = 4096
H = 32
KV = 8
HD = 128
FF = 14336
GROUP = H // KV
PER_DEV = KV // TP
QBLOCK = min(S, 512)
NORM_EPS = 1e-5
ROPE_BASE = 10000.0


def to_dec_order(tensor, head_axis):
    arr_dims = tensor.shape
    split_heads = tensor.reshape(arr_dims[:head_axis] + (PER_DEV, TP) + arr_dims[head_axis + 1:])
    return jnp.swapaxes(split_heads, head_axis, head_axis + 1).reshape(arr_dims)


def setup_inputs(seed: int = 0, part: int = 0) -> dict:
    root_key = jax.random.key(seed)
    keys_part = jax.random.split(jax.random.fold_in(root_key, part), 6)
    keys_shared = jax.random.split(jax.random.fold_in(root_key, 100003), 7)
    prompt = jax.random.normal(keys_part[0], (NODE, S, D), jnp.float32).astype(jnp.bfloat16)
    s_len = jax.random.randint(keys_part[1], (NODE,), (3 * S) // 4, S + 1, dtype=jnp.int32)
    s_len = s_len.at[0].set(S).at[NODE - 1].set((3 * S) // 4)
    tokens = jax.random.normal(keys_part[2], (NODE, BD, D), jnp.float32).astype(jnp.bfloat16)
    c_len = jax.random.randint(keys_part[3], (NODE, BD), T // 2, T, dtype=jnp.int32)
    c_len = c_len.at[0, 0].set(T - 1).at[0, 1].set(T // 2)
    k_cache = jax.random.normal(keys_part[4], (L, NODE, BD, T, KV, HD), jnp.float32).astype(jnp.bfloat16)
    v_cache = jax.random.normal(keys_part[5], (L, NODE, BD, T, KV, HD), jnp.float32).astype(jnp.bfloat16)
    attn_norm = jax.random.uniform(keys_shared[0], (L, D), jnp.float32, 0.5, 1.5).astype(jnp.bfloat16)
    mlp_norm = jax.random.uniform(keys_shared[1], (L, D), jnp.float32, 0.5, 1.5).astype(jnp.bfloat16)
    w_qkv = (jax.random.normal(keys_shared[2], (L, D, KV, GROUP + 2, HD), jnp.float32) * D ** -0.5).astype(jnp.bfloat16)
    w_out = (jax.random.normal(keys_shared[3], (L, KV, GROUP, HD, D), jnp.float32) * (H * HD) ** -0.5).astype(jnp.bfloat16)
    w_gate = (jax.random.normal(keys_shared[4], (L, D, FF), jnp.float32) * D ** -0.5).astype(jnp.bfloat16)
    w_up = (jax.random.normal(keys_shared[5], (L, D, FF), jnp.float32) * D ** -0.5).astype(jnp.bfloat16)
    w_down = (jax.random.normal(keys_shared[6], (L, FF, D), jnp.float32) * FF ** -0.5).astype(jnp.bfloat16)
    return {'prompt': prompt, 's_len': s_len, 'tokens': tokens, 'c_len': c_len, 'k_cache': k_cache, 'v_cache': v_cache, 'attn_norm': attn_norm, 'mlp_norm': mlp_norm, 'w_qkv_pre': w_qkv, 'w_out_pre': w_out, 'w_qkv_dec': to_dec_order(w_qkv, 2), 'w_out_dec': to_dec_order(w_out, 1), 'w_gate': w_gate, 'w_up': w_up, 'w_down': w_down}


def rope_tables(positions):
    inv_freq = jnp.exp(jnp.arange(HD // 2, dtype=jnp.float32) * (-2.0 * math.log(ROPE_BASE) / HD))
    angles = positions.astype(jnp.float32)[..., None] * inv_freq
    return jnp.cos(angles), jnp.sin(angles)


def apply_rope(vectors, cos_tab, sin_tab):
    vec32 = vectors.astype(jnp.float32)
    first_half = vec32[..., :HD // 2]
    second_half = vec32[..., HD // 2:]
    return jnp.concatenate([first_half * cos_tab - second_half * sin_tab, second_half * cos_tab + first_half * sin_tab], axis=-1).astype(jnp.bfloat16)


def rms_norm(hidden, gain_vec):
    hidden_f = hidden.astype(jnp.float32)
    inv_rms = lax.rsqrt(jnp.mean(hidden_f * hidden_f, axis=-1, keepdims=True) + NORM_EPS)
    return (hidden_f * inv_rms * gain_vec.astype(jnp.float32)).astype(jnp.bfloat16)


def residual_add(hidden, delta_bf):
    return (hidden.astype(jnp.float32) + delta_bf.astype(jnp.float32)).astype(jnp.bfloat16)


def mlp_block(hidden, gain_mlp, gate_mat, up_mat, down_mat):
    normed = rms_norm(hidden, gain_mlp)
    gate_act = jnp.dot(normed, gate_mat, preferred_element_type=jnp.float32).astype(jnp.bfloat16)
    up_proj = jnp.dot(normed, up_mat, preferred_element_type=jnp.float32).astype(jnp.bfloat16)
    swi_act = (jax.nn.silu(gate_act.astype(jnp.float32)) * up_proj.astype(jnp.float32)).astype(jnp.bfloat16)
    down_out = jnp.dot(swi_act, down_mat, preferred_element_type=jnp.float32).astype(jnp.bfloat16)
    return residual_add(hidden, down_out)


def prefill_node(prompt_rows, valid_len, attn_norm, mlp_norm, w_qkv, w_out, w_gate, w_up, w_down):
    positions = jnp.arange(S)
    cos_tab, sin_tab = rope_tables(positions)
    key_ok = positions < valid_len
    allowed = (positions[None, :] <= positions[:, None]) & key_ok[None, :]

    def layer_step(hidden, weights):
        gain_attn, gain_mlp, qkv_mat, out_mat, gate_mat, up_mat, down_mat = weights
        normed = rms_norm(hidden, gain_attn)
        qkv_all = jnp.dot(normed, qkv_mat.reshape(D, KV * (GROUP + 2) * HD), preferred_element_type=jnp.float32).astype(jnp.bfloat16).reshape(S, KV, GROUP + 2, HD)
        q_rot = apply_rope(qkv_all[:, :, :GROUP], cos_tab[:, None, None, :], sin_tab[:, None, None, :])
        k_rot = apply_rope(qkv_all[:, :, GROUP], cos_tab[:, None, :], sin_tab[:, None, :])
        v_new = qkv_all[:, :, GROUP + 1]
        k_f32 = k_rot.astype(jnp.float32)
        v_f32 = v_new.astype(jnp.float32)

        def attend(q_start):
            q_block = lax.dynamic_slice_in_dim(q_rot, q_start, QBLOCK, axis=0).astype(jnp.float32)
            scores = jnp.einsum('qkgd,tkd->kgqt', q_block, k_f32) * (HD ** -0.5)
            mask_rows = lax.dynamic_slice_in_dim(allowed, q_start, QBLOCK, axis=0)
            scores = jnp.where(mask_rows[None, None], scores, -1e30)
            probs_bf = jax.nn.softmax(scores, axis=-1).astype(jnp.bfloat16)
            return jnp.einsum('kgqt,tkd->qkgd', probs_bf.astype(jnp.float32), v_f32).astype(jnp.bfloat16)

        context = lax.map(attend, jnp.arange(S // QBLOCK) * QBLOCK).reshape(S, KV, GROUP, HD)
        attn_out = jnp.einsum('skgd,kgde->se', context.astype(jnp.float32), out_mat.astype(jnp.float32)).astype(jnp.bfloat16)
        hidden = residual_add(hidden, attn_out)
        hidden = mlp_block(hidden, gain_mlp, gate_mat, up_mat, down_mat)
        keep_mask = key_ok[:, None, None]
        return hidden, (jnp.where(keep_mask, k_rot, jnp.zeros_like(k_rot)), jnp.where(keep_mask, v_new, jnp.zeros_like(v_new)))

    return lax.scan(layer_step, prompt_rows, (attn_norm, mlp_norm, w_qkv, w_out, w_gate, w_up, w_down))


def decode_node(tok_rows, lengths, k_layers, v_layers, attn_norm, mlp_norm, w_qkv, w_out, w_gate, w_up, w_down):
    cos_tab, sin_tab = rope_tables(lengths)
    cache_pos = jnp.arange(T)
    write_mask = cache_pos[None, :] == lengths[:, None]
    seen_mask = cache_pos[None, :] <= lengths[:, None]

    def layer_step(hidden, weights):
        gain_attn, gain_mlp, qkv_mat, out_mat, gate_mat, up_mat, down_mat, k_old, v_old = weights
        normed = rms_norm(hidden, gain_attn)
        qkv_all = jnp.dot(normed, qkv_mat.reshape(D, KV * (GROUP + 2) * HD), preferred_element_type=jnp.float32).astype(jnp.bfloat16).reshape(BD, KV, GROUP + 2, HD)
        q_rot = apply_rope(qkv_all[:, :, :GROUP], cos_tab[:, None, None, :], sin_tab[:, None, None, :])
        k_rot = apply_rope(qkv_all[:, :, GROUP], cos_tab[:, None, :], sin_tab[:, None, :])
        v_new = qkv_all[:, :, GROUP + 1]
        k_upd = jnp.where(write_mask[:, :, None, None], k_rot[:, None], k_old)
        v_upd = jnp.where(write_mask[:, :, None, None], v_new[:, None], v_old)
        scores = jnp.einsum('bkgd,btkd->bkgt', q_rot.astype(jnp.float32), k_upd.astype(jnp.float32)) * (HD ** -0.5)
        scores = jnp.where(seen_mask[:, None, None, :], scores, -1e30)
        probs_bf = jax.nn.softmax(scores, axis=-1).astype(jnp.bfloat16)
        context = jnp.einsum('bkgt,btkd->bkgd', probs_bf.astype(jnp.float32), v_upd.astype(jnp.float32)).astype(jnp.bfloat16)
        attn_out = jnp.einsum('bkgd,kgde->be', context.astype(jnp.float32), out_mat.astype(jnp.float32)).astype(jnp.bfloat16)
        hidden = residual_add(hidden, attn_out)
        hidden = mlp_block(hidden, gain_mlp, gate_mat, up_mat, down_mat)
        return hidden, (k_upd, v_upd)

    return lax.scan(layer_step, tok_rows, (attn_norm, mlp_norm, w_qkv, w_out, w_gate, w_up, w_down, k_layers, v_layers))


def reference(prompt, s_len, tokens, c_len, k_cache, v_cache, attn_norm, mlp_norm, w_qkv_pre, w_out_pre, w_qkv_dec, w_out_dec, w_gate, w_up, w_down):
    def run_prefill(node_args):
        prompt_rows, valid_len = node_args
        return prefill_node(prompt_rows, valid_len, attn_norm, mlp_norm, w_qkv_pre, w_out_pre, w_gate, w_up, w_down)

    hidden, (k_made, v_made) = lax.map(run_prefill, (prompt, s_len))
    k_prompt = jnp.roll(to_dec_order(k_made, 3), NODE // 2, axis=0).transpose(1, 0, 2, 3, 4)
    v_prompt = jnp.roll(to_dec_order(v_made, 3), NODE // 2, axis=0).transpose(1, 0, 2, 3, 4)

    def run_decode(node_args):
        tok_rows, lengths, k_layers, v_layers = node_args
        return decode_node(tok_rows, lengths, k_layers, v_layers, attn_norm, mlp_norm, w_qkv_dec, w_out_dec, w_gate, w_up, w_down)

    tok_out, (k_new, v_new) = lax.map(run_decode, (tokens, c_len, jnp.swapaxes(k_cache, 0, 1), jnp.swapaxes(v_cache, 0, 1)))
    return (hidden, tok_out, k_prompt, v_prompt, jnp.swapaxes(k_new, 0, 1), jnp.swapaxes(v_new, 0, 1))
```

```python
import functools
import math
import jax
import jax.numpy as jnp
from jax import lax
from jax.experimental import pallas as pl
from jax.experimental.pallas import tpu as pltpu
from jax.sharding import PartitionSpec as P

NORM_EPS = 1e-5
ROPE_BASE = 10000.0
CHUNKS = 4
F32 = jnp.float32
BF16 = jnp.bfloat16


def rope_tables(positions, head_dim):
    inv_freq = jnp.exp(jnp.arange(head_dim // 2, dtype=F32) * (-2.0 * math.log(ROPE_BASE) / head_dim))
    angles = positions.astype(F32)[..., None] * inv_freq
    return jnp.cos(angles), jnp.sin(angles)


def apply_rope(vectors, cos_tab, sin_tab):
    half_dim = vectors.shape[-1] // 2
    vec32 = vectors.astype(F32)
    first_half = vec32[..., :half_dim]
    second_half = vec32[..., half_dim:]
    return jnp.concatenate([first_half * cos_tab - second_half * sin_tab, second_half * cos_tab + first_half * sin_tab], axis=-1).astype(BF16)


def rms_norm(hidden, gain_vec):
    hidden_f = hidden.astype(F32)
    inv_rms = lax.rsqrt(jnp.mean(hidden_f * hidden_f, axis=-1, keepdims=True) + NORM_EPS)
    return (hidden_f * inv_rms * gain_vec.astype(F32)).astype(BF16)


def residual_add(hidden, delta_bf):
    return (hidden.astype(F32) + delta_bf.astype(F32)).astype(BF16)


def dot32(a, b):
    return jnp.dot(a, b, preferred_element_type=F32)


def kv_prep_kernel(slen_ref, *refs, kv_local, head_dim, rows):
    k_refs = refs[:kv_local]
    v_refs = refs[kv_local:2 * kv_local]
    cos_ref, sin_ref, k_out, pack_out = refs[2 * kv_local:]
    pos = pl.program_id(0) * rows + lax.broadcasted_iota(jnp.int32, (rows, head_dim), 0)
    keep = pos < slen_ref[0]
    for head in range(kv_local):
        k32 = k_refs[head][...].astype(F32)
        k_rot = (k32 * cos_ref[...] + pltpu.roll(k32, head_dim // 2, 1) * sin_ref[...]).astype(BF16)
        k_out[:, head * head_dim:(head + 1) * head_dim] = k_rot
        zero = jnp.zeros_like(k_rot)
        pack_out[head, 0] = jnp.where(keep, k_rot, zero)
        pack_out[head, 1] = jnp.where(keep, v_refs[head][...], zero)


def kv_prep(qkv, s_len, cos_full, sin_full, kv_local, group_size, head_dim):
    seq_len = qkv.shape[0]
    rows = 512
    per_kv = group_size + 2
    col = lambda c: pl.BlockSpec((rows, head_dim), lambda r, c=c: (r, c))
    in_specs = [pl.BlockSpec(memory_space=pltpu.SMEM)]
    in_specs += [col(h * per_kv + group_size) for h in range(kv_local)]
    in_specs += [col(h * per_kv + group_size + 1) for h in range(kv_local)]
    in_specs += [col(0), col(0)]
    return pl.pallas_call(
        functools.partial(kv_prep_kernel, kv_local=kv_local, head_dim=head_dim, rows=rows),
        grid=(seq_len // rows,),
        in_specs=in_specs,
        out_specs=[pl.BlockSpec((rows, kv_local * head_dim), lambda r: (r, 0)), pl.BlockSpec((kv_local, 2, rows, head_dim), lambda r: (0, 0, r, 0))],
        out_shape=[jax.ShapeDtypeStruct((seq_len, kv_local * head_dim), BF16), jax.ShapeDtypeStruct((kv_local, 2, seq_len, head_dim), BF16)],
        cost_estimate=pl.CostEstimate(flops=seq_len * 4096, bytes_accessed=seq_len * 3072, transcendentals=0),
        name="kv_prep",
    )(s_len, *([qkv] * (2 * kv_local)), cos_full, sin_full)


def attend_kernel(slen_ref, q_ref, cos_ref, sin_ref, k_ref, v_ref, out_ref, *, start, rows, sub):
    head_dim = q_ref.shape[1]
    scale = (head_dim ** -0.5) * math.log2(math.e)
    q32 = q_ref[...].astype(F32)
    q_rot = (q32 * cos_ref[...] + pltpu.roll(q32, head_dim // 2, 1) * sin_ref[...]).astype(BF16)
    dims = (((1,), (1,)), ((), ()))
    for part in range(rows // sub):
        q_part = q_rot[part * sub:(part + 1) * sub]
        base = start + part * sub
        width = base + sub
        tail = lax.dot_general(q_part, k_ref[base:width], dims, preferred_element_type=F32)
        q_pos = lax.broadcasted_iota(jnp.int32, (sub, sub), 0)
        k_pos = lax.broadcasted_iota(jnp.int32, (sub, sub), 1)
        allowed = (k_pos <= q_pos) & (k_pos + base < slen_ref[0])
        tail = jnp.where(allowed, tail, -1e30)
        top = jnp.max(tail, axis=1, keepdims=True)
        if base > 0:
            body = lax.dot_general(q_part, k_ref[:base], dims, preferred_element_type=F32)
            safe = 1536
            if base > safe:
                k_head = lax.broadcasted_iota(jnp.int32, (sub, base - safe), 1) + safe
                late = jnp.where(k_head < slen_ref[0], body[:, safe:], -1e30)
                body = jnp.concatenate([body[:, :safe], late], axis=1)
            top = jnp.maximum(top, jnp.max(body, axis=1, keepdims=True))
            p_body = jnp.exp2((body - top) * scale)
            p_tail = jnp.exp2((tail - top) * scale)
            inv = 1.0 / (jnp.sum(p_body, axis=1, keepdims=True) + jnp.sum(p_tail, axis=1, keepdims=True))
            acc = dot32((p_body * inv).astype(BF16), v_ref[:base]) + dot32((p_tail * inv).astype(BF16), v_ref[base:width])
        else:
            p_tail = jnp.exp2((tail - top) * scale)
            inv = 1.0 / jnp.sum(p_tail, axis=1, keepdims=True)
            acc = dot32((p_tail * inv).astype(BF16), v_ref[base:width])
        out_ref[part * sub:(part + 1) * sub, :] = acc.astype(BF16)


def attend_chunk(qkv, k_rot, cos_full, sin_full, s_len, chunk, rows, kv_local, group_size, head_dim):
    heads = kv_local * group_size
    per_kv = group_size + 2
    width = (chunk + 1) * rows
    tab = pl.BlockSpec((rows, head_dim), lambda h: (chunk, 0))
    return pl.pallas_call(
        functools.partial(attend_kernel, start=chunk * rows, rows=rows, sub=256),
        grid=(heads,),
        in_specs=[
            pl.BlockSpec(memory_space=pltpu.SMEM),
            pl.BlockSpec((rows, head_dim), lambda h: (chunk, (h // group_size) * per_kv + h % group_size)),
            tab,
            tab,
            pl.BlockSpec((width, head_dim), lambda h: (0, h // group_size)),
            pl.BlockSpec((width, head_dim), lambda h: (0, (h // group_size) * per_kv + group_size + 1)),
        ],
        out_specs=pl.BlockSpec((rows, head_dim), lambda h: (0, h)),
        out_shape=jax.ShapeDtypeStruct((rows, heads * head_dim), BF16),
        cost_estimate=pl.CostEstimate(flops=4 * rows * width * heads * head_dim * 3, bytes_accessed=4 * rows * heads * head_dim, transcendentals=rows * width * heads),
        name="attend",
    )(s_len, qkv, cos_full, sin_full, k_rot, qkv)


def project_kernel(place_ref, *refs, tp_count, n_in):
    ctx_refs = refs[:n_in]
    w_ref, x_ref, h_ref, ctx_all = refs[n_in:]

    @pl.when(pl.program_id(0) == 0)
    def _():
        if n_in == 1:
            ctx_all[...] = ctx_refs[0][...]
        else:
            own, succ, far_a, far_b, prev = ctx_refs
            me = place_ref[0]
            half = far_a.shape[0]
            ctx_all[me] = own[...]
            ctx_all[lax.rem(me + 1, tp_count)] = succ[...]
            ctx_all[lax.rem(me + 2, tp_count), :half] = far_a[...]
            ctx_all[lax.rem(me + 2, tp_count), half:] = far_b[...]
            ctx_all[lax.rem(me + 3, tp_count)] = prev[...]

    depth = ctx_all.shape[2]
    acc = dot32(ctx_all[0], w_ref[:depth])
    for block in range(1, tp_count):
        acc += dot32(ctx_all[block], w_ref[block * depth:(block + 1) * depth])
    h_ref[...] = (x_ref[...].astype(F32) + acc.astype(BF16).astype(F32)).astype(BF16)


def project_chunk(ctx_parts, out_full, x, row_block, rows, place, tp_count, tile=512):
    full_depth, width = out_full.shape
    depth = full_depth // tp_count
    whole = lambda part: pl.BlockSpec(part.shape, lambda j: (0,) * part.ndim, pipeline_mode=pl.Buffered(1))
    return pl.pallas_call(
        functools.partial(project_kernel, tp_count=tp_count, n_in=len(ctx_parts)),
        grid=(width // tile,),
        in_specs=[pl.BlockSpec(memory_space=pltpu.SMEM)] + [whole(p) for p in ctx_parts] + [
            pl.BlockSpec((full_depth, tile), lambda j: (0, j)),
            pl.BlockSpec((rows, tile), lambda j: (row_block, j)),
        ],
        out_specs=pl.BlockSpec((rows, tile), lambda j: (0, j)),
        out_shape=jax.ShapeDtypeStruct((rows, width), BF16),
        scratch_shapes=[pltpu.VMEM((tp_count, rows, depth), BF16)],
        compiler_params=pltpu.CompilerParams(vmem_limit_bytes=40 * 1024 * 1024),
        cost_estimate=pl.CostEstimate(flops=2 * rows * full_depth * width, bytes_accessed=2 * full_depth * width, transcendentals=0),
        name="project",
    )(place, *ctx_parts, out_full, x)


def mlp_kernel(h_ref, gain_ref, wg_ref, wu_ref, wd_ref, out_ref, m_ref):
    step = pl.program_id(0)
    rows, _ = h_ref.shape
    sub = min(rows, 128)

    @pl.when(step == 0)
    def _():
        @pl.loop(0, rows // sub)
        def _(part):
            at = pl.ds(pl.multiple_of(part * sub, sub), sub)
            h32 = h_ref[at, :].astype(F32)
            inv_rms = lax.rsqrt(jnp.mean(h32 * h32, axis=-1, keepdims=True) + NORM_EPS)
            m_ref[at, :] = (h32 * inv_rms * gain_ref[...].astype(F32)).astype(BF16)

    gate_act = dot32(m_ref[...], wg_ref[...]).astype(BF16).astype(F32)
    up_proj = dot32(m_ref[...], wu_ref[...]).astype(BF16).astype(F32)
    swi_act = (jax.nn.silu(gate_act) * up_proj).astype(BF16)

    @pl.when(step == 0)
    def _():
        out_ref[...] = dot32(swi_act, wd_ref[...])

    @pl.when(step > 0)
    def _():
        out_ref[...] += dot32(swi_act, wd_ref[...])


def mlp_chunk(hidden, gain, gate_mat, up_mat, down_mat, tile=512):
    rows, width = hidden.shape
    ff = gate_mat.shape[1]
    once = lambda shape: pl.BlockSpec(shape, lambda f: (0, 0), pipeline_mode=pl.Buffered(1))
    return pl.pallas_call(
        mlp_kernel,
        grid=(ff // tile,),
        in_specs=[
            once((rows, width)),
            once((1, width)),
            pl.BlockSpec((width, tile), lambda f: (0, f)),
            pl.BlockSpec((width, tile), lambda f: (0, f)),
            pl.BlockSpec((tile, width), lambda f: (f, 0)),
        ],
        out_specs=pl.BlockSpec((rows, width), lambda f: (0, 0), pipeline_mode=pl.Buffered(1)),
        out_shape=jax.ShapeDtypeStruct((rows, width), F32),
        scratch_shapes=[pltpu.VMEM((rows, width), BF16)],
        compiler_params=pltpu.CompilerParams(vmem_limit_bytes=60 * 1024 * 1024),
        cost_estimate=pl.CostEstimate(flops=6 * rows * width * ff, bytes_accessed=6 * width * ff, transcendentals=rows * ff),
        name="mlp",
    )(hidden, gain, gate_mat, up_mat, down_mat)


def after(value, *deps):
    return lax.optimization_barrier((value,) + deps)[0]


def make_ring(tp_count):
    up = [(i, (i + 1) % tp_count) for i in range(tp_count)]
    down = [((i + 1) % tp_count, i) for i in range(tp_count)]
    return (lambda x: lax.ppermute(x, 'tp', up)), (lambda x: lax.ppermute(x, 'tp', down))


def ring_gather(block, tp_count):
    send_up, send_down = make_ring(tp_count)
    half = block.shape[0] // 2
    prev = send_up(block)
    succ = send_down(block)
    return [block, succ, send_up(prev[:half]), send_down(succ[half:]), prev]


def scatter_first(partial, tp_count, me):
    send_up, send_down = make_ring(tp_count)
    half = partial.shape[1] // 2
    far_at = (me + 2) % tp_count
    width = partial.shape[2]
    lower = lax.dynamic_slice(partial, (far_at, 0, 0), (1, half, width))[0]
    upper = lax.dynamic_slice(partial, (far_at, half, 0), (1, half, width))[0]
    from_prev = send_up(lower)
    from_succ = send_down(upper)
    return from_prev, from_succ


def scatter_add(partial, first, tp_count, me):
    from_prev, from_succ = first
    half = partial.shape[1] // 2
    pick = lambda dist: lax.dynamic_index_in_dim(partial, (me + dist) % tp_count, axis=0, keepdims=False)
    succ, prev = pick(1), pick(3)
    up_block = jnp.concatenate([succ[:half] + from_prev, succ[half:]], axis=0)
    down_block = jnp.concatenate([prev[:half], prev[half:] + from_succ], axis=0)
    return up_block, down_block


def scatter_last(partial, blocks, tp_count, me):
    send_up, send_down = make_ring(tp_count)
    own = lax.dynamic_index_in_dim(partial, me, axis=0, keepdims=False)
    from_prev = send_up(blocks[0])
    from_succ = send_down(blocks[1])
    return own + (from_prev + from_succ)


def small_sum(partial, tp_count):
    send_up, send_down = make_ring(tp_count)
    far = lax.ppermute(partial, 'tp', [(i, (i + 2) % tp_count) for i in range(tp_count)])
    return (partial + far) + (send_up(partial) + send_down(partial))


def hand_off(pack, tp_count, node_count, tp_index):
    kv_local = pack.shape[0]
    spread = tp_count // kv_local
    got = []
    for step in range(kv_local):
        head = (tp_index // spread + step) % kv_local
        piece = lax.dynamic_index_in_dim(pack, head, axis=0, keepdims=False)
        pairs = []
        for node in range(node_count):
            for src in range(tp_count):
                h = (src // spread + step) % kv_local
                dst = (src % spread) * kv_local + h
                pairs.append((src * node_count + node, dst * node_count + (node + node_count // 2) % node_count))
        got.append(lax.ppermute(piece, ('tp', 'node'), pairs))
    first = jnp.stack([got[0], got[1]], axis=2)
    second = jnp.stack([got[1], got[0]], axis=2)
    both = jnp.where(tp_index % kv_local == 0, first, second)
    return both[0][None, None], both[1][None, None]


def decode_attention(q_rot, k_rot, v_new, k_old, v_old, write_mask, seen_mask):
    k_upd = jnp.where(write_mask[:, :, :, None, None], k_rot[:, :, None], k_old)
    v_upd = jnp.where(write_mask[:, :, :, None, None], v_new[:, :, None], v_old)
    scores = jnp.einsum('nbkgd,nbtkd->nbkgt', q_rot, k_upd, preferred_element_type=F32) * (q_rot.shape[-1] ** -0.5)
    scores = jnp.where(seen_mask[:, :, None, None, :], scores, -1e30)
    probs_bf = jax.nn.softmax(scores, axis=-1).astype(BF16)
    context = jnp.einsum('nbkgt,nbtkd->nbkgd', probs_bf, v_upd, preferred_element_type=F32).astype(BF16)
    return context, k_upd, v_upd


def mlp_partial(hidden, gain, gate_mat, up_mat, down_mat):
    normed = rms_norm(hidden, gain)
    gate_act = dot32(normed, gate_mat).astype(BF16)
    up_proj = dot32(normed, up_mat).astype(BF16)
    swi_act = (jax.nn.silu(gate_act.astype(F32)) * up_proj.astype(F32)).astype(BF16)
    return dot32(swi_act, down_mat)


def run_decode(tokens, hold, c_len, k_cache, v_cache, attn_gain, mlp_gain, qkv_dec, out_dec, gate_mat, up_mat, down_mat, tp_count):
    group_size = qkv_dec.shape[2] - 2
    cos_tab, sin_tab = rope_tables(c_len, qkv_dec.shape[-1])
    cache_pos = jnp.arange(k_cache.shape[2])
    write_mask = cache_pos[None, None, :] == c_len[:, :, None]
    seen_mask = cache_pos[None, None, :] <= c_len[:, :, None]
    normed = rms_norm(tokens, attn_gain)
    qkv_all = jnp.einsum('nse,ekcd->nskcd', normed, qkv_dec, preferred_element_type=F32).astype(BF16)
    q_rot = apply_rope(qkv_all[:, :, :, :group_size], cos_tab[:, :, None, None, :], sin_tab[:, :, None, None, :])
    k_rot = apply_rope(qkv_all[:, :, :, group_size], cos_tab[:, :, None, :], sin_tab[:, :, None, :])
    context, k_upd, v_upd = decode_attention(q_rot, k_rot, qkv_all[:, :, :, group_size + 1], k_cache, v_cache, write_mask, seen_mask)
    attn_part = jnp.einsum('nskgd,kgde->nse', context, out_dec, preferred_element_type=F32)
    hidden = residual_add(tokens, small_sum(attn_part, tp_count).astype(BF16))
    hidden = after(hidden, hold)
    down_part = mlp_partial(hidden[0], mlp_gain, gate_mat, up_mat, down_mat)[None]
    hidden = residual_add(hidden, small_sum(down_part, tp_count).astype(BF16))
    return hidden, k_upd[None], v_upd[None]


def solution(mesh):
    node_count = mesh.shape['node']
    tp_count = mesh.shape['tp']
    row_spec = P(('pair', 'node'), None, None)
    len_spec = P(('pair', 'node'))
    clen_spec = P(('pair', 'node'), None)
    cache_spec = P(None, ('pair', 'node'), None, None, 'tp', None)
    prompt_kv_spec = P(None, ('pair', 'node'), None, 'tp', None)
    gain_spec = P(None, None)
    qkv_spec = P(None, None, 'tp', None, None)
    out_spec = P(None, 'tp', None, None, None)
    col_spec = P(None, None, 'tp')
    down_spec = P(None, 'tp', None)

    def local_fn(prompt, s_len, tokens, c_len, k_cache, v_cache, attn_norm, mlp_norm, w_qkv_pre, w_out_pre, w_qkv_dec, w_out_dec, w_gate, w_up, w_down):
        tp_index = lax.axis_index('tp')
        node_index = lax.axis_index('node')
        width = prompt.shape[-1]
        seq_len = prompt.shape[1]
        kv_local, per_kv, head_dim = w_qkv_pre.shape[2:]
        group_size = per_kv - 2
        gate_mat, up_mat, down_mat = w_gate[0], w_up[0], w_down[0]

        out_local = w_out_pre[0].reshape(kv_local * group_size * head_dim, width)
        slice_rows = out_local.shape[0] // node_count
        out_slice = lax.dynamic_slice_in_dim(out_local, node_index * slice_rows, slice_rows, axis=0)
        out_full = lax.all_gather(out_slice, ('tp', 'node'), axis=0, tiled=True)

        x = prompt[0]
        qkv = dot32(rms_norm(x, attn_norm[0]), w_qkv_pre[0].reshape(width, kv_local * per_kv * head_dim)).astype(BF16)
        cos_tab, sin_tab = rope_tables(jnp.arange(seq_len), head_dim)
        cos_full = jnp.concatenate([cos_tab, cos_tab], axis=-1)
        sin_full = jnp.concatenate([-sin_tab, sin_tab], axis=-1)
        k_rot, pack = kv_prep(qkv, s_len, cos_full, sin_full, kv_local, group_size, head_dim)

        rows = seq_len // CHUNKS
        own_rows = rows // tp_count
        place = tp_index.astype(jnp.int32)[None]
        contexts = [attend_chunk(qkv, k_rot, cos_full, sin_full, s_len, c, rows, kv_local, group_size, head_dim) for c in range(CHUNKS)]
        ctx_parts = [ring_gather(contexts[0], tp_count)]
        ctx_parts += [[lax.all_gather(context, 'tp', axis=0)] for context in contexts[1:]]
        partials, blocks, finals, hiddens, firsts = [], [], [], [], []

        def finish(c):
            summed = scatter_last(partials[c], blocks[c], tp_count, tp_index)
            own_hidden = lax.dynamic_slice_in_dim(hiddens[c], tp_index * own_rows, own_rows, axis=0)
            finals.append(residual_add(own_hidden, summed.astype(BF16)))

        for chunk in range(CHUNKS):
            deps = []
            if chunk >= 2:
                finish(chunk - 2)
                deps.append(finals[chunk - 2])
            if chunk >= 1:
                deps.append(partials[chunk - 1])
            parts = ctx_parts[chunk]
            if deps:
                parts = list(lax.optimization_barrier(tuple(parts) + tuple(deps))[:len(parts)])
            hidden = project_chunk(parts, out_full, x, chunk, rows, place, tp_count)
            if chunk >= 1:
                blocks.append(scatter_add(partials[chunk - 1], firsts[chunk - 1], tp_count, tp_index))
                hidden = after(hidden, *blocks[chunk - 1])
            hiddens.append(hidden)
            partial = mlp_chunk(hidden, mlp_norm, gate_mat, up_mat, down_mat).reshape(tp_count, own_rows, width)
            partials.append(partial)
            firsts.append(scatter_first(partial, tp_count, tp_index))
        finish(CHUNKS - 2)
        blocks.append(scatter_add(partials[-1], firsts[-1], tp_count, tp_index))
        finish(CHUNKS - 1)
        out = jnp.concatenate([lax.all_gather(final, 'tp', axis=0, tiled=True) for final in finals], axis=0)

        k_prompt, v_prompt = hand_off(pack, tp_count, node_count, tp_index)
        tok_out, k_new, v_new = run_decode(after(tokens, partials[CHUNKS - 1]), partials[CHUNKS - 1], c_len, k_cache[0], v_cache[0], attn_norm[0], mlp_norm[0], w_qkv_dec[0], w_out_dec[0], gate_mat, up_mat, down_mat, tp_count)
        return out[None], tok_out, k_prompt, v_prompt, k_new, v_new

    return jax.shard_map(local_fn, mesh=mesh, in_specs=(row_spec, len_spec, row_spec, clen_spec, cache_spec, cache_spec, gain_spec, gain_spec, qkv_spec, out_spec, qkv_spec, out_spec, col_spec, col_spec, down_spec), out_specs=(row_spec, row_spec, prompt_kv_spec, prompt_kv_spec, cache_spec, cache_spec), check_vma=False)
```

```python
import functools
import math
import jax
import jax.numpy as jnp
from jax import lax
from jax.experimental import pallas as pl
from jax.experimental.pallas import tpu as pltpu
from jax.sharding import PartitionSpec as P

NORM_EPS = 1e-5
ROPE_BASE = 10000.0
EDGE_ROWS = 256
MID_ROWS = 512
F32 = jnp.float32
BF16 = jnp.bfloat16


def chunk_edges(seq_len):
    return [0] + list(range(EDGE_ROWS, seq_len, MID_ROWS)) + [seq_len]


def rope_tables(positions, head_dim):
    inv_freq = jnp.exp(jnp.arange(head_dim // 2, dtype=F32) * (-2.0 * math.log(ROPE_BASE) / head_dim))
    angles = positions.astype(F32)[..., None] * inv_freq
    return jnp.cos(angles), jnp.sin(angles)


def apply_rope(vectors, cos_tab, sin_tab):
    half_dim = vectors.shape[-1] // 2
    vec32 = vectors.astype(F32)
    first_half = vec32[..., :half_dim]
    second_half = vec32[..., half_dim:]
    return jnp.concatenate([first_half * cos_tab - second_half * sin_tab, second_half * cos_tab + first_half * sin_tab], axis=-1).astype(BF16)


def rms_norm(hidden, gain_vec):
    hidden_f = hidden.astype(F32)
    inv_rms = lax.rsqrt(jnp.mean(hidden_f * hidden_f, axis=-1, keepdims=True) + NORM_EPS)
    return (hidden_f * inv_rms * gain_vec.astype(F32)).astype(BF16)


def residual_add(hidden, delta_bf):
    return (hidden.astype(F32) + delta_bf.astype(F32)).astype(BF16)


def dot32(a, b):
    return jnp.dot(a, b, preferred_element_type=F32)


def kv_prep_kernel(slen_ref, *refs, kv_local, head_dim, rows):
    k_refs = refs[:kv_local]
    v_refs = refs[kv_local:2 * kv_local]
    cos_ref, sin_ref, k_out, pack_out = refs[2 * kv_local:]
    pos = pl.program_id(0) * rows + lax.broadcasted_iota(jnp.int32, (rows, head_dim), 0)
    keep = pos < slen_ref[0]
    for head in range(kv_local):
        k32 = k_refs[head][...].astype(F32)
        k_rot = (k32 * cos_ref[...] + pltpu.roll(k32, head_dim // 2, 1) * sin_ref[...]).astype(BF16)
        k_out[:, head * head_dim:(head + 1) * head_dim] = k_rot
        zero = jnp.zeros_like(k_rot)
        pack_out[head, 0] = jnp.where(keep, k_rot, zero)
        pack_out[head, 1] = jnp.where(keep, v_refs[head][...], zero)


def kv_prep(qkv, s_len, cos_full, sin_full, kv_local, group_size, head_dim):
    seq_len = qkv.shape[0]
    rows = 512
    per_kv = group_size + 2
    col = lambda c: pl.BlockSpec((rows, head_dim), lambda r, c=c: (r, c))
    in_specs = [pl.BlockSpec(memory_space=pltpu.SMEM)]
    in_specs += [col(h * per_kv + group_size) for h in range(kv_local)]
    in_specs += [col(h * per_kv + group_size + 1) for h in range(kv_local)]
    in_specs += [col(0), col(0)]
    return pl.pallas_call(
        functools.partial(kv_prep_kernel, kv_local=kv_local, head_dim=head_dim, rows=rows),
        grid=(seq_len // rows,),
        in_specs=in_specs,
        out_specs=[pl.BlockSpec((rows, kv_local * head_dim), lambda r: (r, 0)), pl.BlockSpec((kv_local, 2, rows, head_dim), lambda r: (0, 0, r, 0))],
        out_shape=[jax.ShapeDtypeStruct((seq_len, kv_local * head_dim), BF16), jax.ShapeDtypeStruct((kv_local, 2, seq_len, head_dim), BF16)],
        cost_estimate=pl.CostEstimate(flops=seq_len * 4096, bytes_accessed=seq_len * 3072, transcendentals=0),
        name="kv_prep",
    )(s_len, *([qkv] * (2 * kv_local)), cos_full, sin_full)


def attend_kernel(slen_ref, *refs, start, sub, n_q):
    q_refs, cos_refs, sin_refs = refs[:n_q], refs[n_q:2 * n_q], refs[2 * n_q:3 * n_q]
    k_ref, v_ref, out_ref = refs[3 * n_q:]
    head_dim = k_ref.shape[1]
    scale = (head_dim ** -0.5) * math.log2(math.e)
    dims = (((1,), (1,)), ((), ()))
    for part in range(n_q):
        q32 = q_refs[part][...].astype(F32)
        q_part = (q32 * cos_refs[part][...] + pltpu.roll(q32, head_dim // 2, 1) * sin_refs[part][...]).astype(BF16)
        base = start + part * sub
        width = base + sub
        tail = lax.dot_general(q_part, k_ref[base:width], dims, preferred_element_type=F32)
        q_pos = lax.broadcasted_iota(jnp.int32, (sub, sub), 0)
        k_pos = lax.broadcasted_iota(jnp.int32, (sub, sub), 1)
        allowed = (k_pos <= q_pos) & (k_pos + base < slen_ref[0])
        tail = jnp.where(allowed, tail, -1e30)
        top = jnp.max(tail, axis=1, keepdims=True)
        if base > 0:
            body = lax.dot_general(q_part, k_ref[:base], dims, preferred_element_type=F32)
            safe = 1536
            if base > safe:
                k_head = lax.broadcasted_iota(jnp.int32, (sub, base - safe), 1) + safe
                late = jnp.where(k_head < slen_ref[0], body[:, safe:], -1e30)
                body = jnp.concatenate([body[:, :safe], late], axis=1)
            top = jnp.maximum(top, jnp.max(body, axis=1, keepdims=True))
            p_body = jnp.exp2((body - top) * scale)
            p_tail = jnp.exp2((tail - top) * scale)
            inv = 1.0 / (jnp.sum(p_body, axis=1, keepdims=True) + jnp.sum(p_tail, axis=1, keepdims=True))
            acc = dot32((p_body * inv).astype(BF16), v_ref[:base]) + dot32((p_tail * inv).astype(BF16), v_ref[base:width])
        else:
            p_tail = jnp.exp2((tail - top) * scale)
            inv = 1.0 / jnp.sum(p_tail, axis=1, keepdims=True)
            acc = dot32((p_tail * inv).astype(BF16), v_ref[base:width])
        out_ref[part * sub:(part + 1) * sub, :] = acc.astype(BF16)


def attend_chunk(qkv, k_rot, cos_full, sin_full, s_len, start, rows, kv_local, group_size, head_dim, sub=256):
    heads = kv_local * group_size
    per_kv = group_size + 2
    width = start + rows
    n_q = rows // sub
    first = start // sub
    tabs = [pl.BlockSpec((sub, head_dim), lambda h, r=r: (first + r, 0)) for r in range(n_q)]
    return pl.pallas_call(
        functools.partial(attend_kernel, start=start, sub=sub, n_q=n_q),
        grid=(heads,),
        in_specs=[pl.BlockSpec(memory_space=pltpu.SMEM)]
        + [pl.BlockSpec((sub, head_dim), lambda h, r=r: (first + r, (h // group_size) * per_kv + h % group_size)) for r in range(n_q)]
        + tabs + tabs + [
            pl.BlockSpec((width, head_dim), lambda h: (0, h // group_size)),
            pl.BlockSpec((width, head_dim), lambda h: (0, (h // group_size) * per_kv + group_size + 1)),
        ],
        out_specs=pl.BlockSpec((rows, head_dim), lambda h: (0, h)),
        out_shape=jax.ShapeDtypeStruct((rows, heads * head_dim), BF16),
        cost_estimate=pl.CostEstimate(flops=4 * rows * width * heads * head_dim * 3, bytes_accessed=4 * rows * heads * head_dim, transcendentals=rows * width * heads),
        name="attend",
    )(s_len, *([qkv] * n_q), *([cos_full] * n_q), *([sin_full] * n_q), k_rot, qkv)


def project_kernel(place_ref, *refs, tp_count, n_in, n_x):
    ctx_refs = refs[:n_in]
    w_ref = refs[n_in]
    x_refs = refs[n_in + 1:n_in + 1 + n_x]
    h_ref, ctx_all = refs[n_in + 1 + n_x:]

    @pl.when(pl.program_id(0) == 0)
    def _():
        if n_in == 1:
            ctx_all[...] = ctx_refs[0][...]
        else:
            own, succ, far_a, far_b, prev = ctx_refs
            me = place_ref[0]
            half = far_a.shape[0]
            ctx_all[me] = own[...]
            ctx_all[lax.rem(me + 1, tp_count)] = succ[...]
            ctx_all[lax.rem(me + 2, tp_count), :half] = far_a[...]
            ctx_all[lax.rem(me + 2, tp_count), half:] = far_b[...]
            ctx_all[lax.rem(me + 3, tp_count)] = prev[...]

    depth = ctx_all.shape[2]
    acc = dot32(ctx_all[0], w_ref[:depth])
    for block in range(1, tp_count):
        acc += dot32(ctx_all[block], w_ref[block * depth:(block + 1) * depth])
    sub = x_refs[0].shape[0]
    for part in range(n_x):
        at = slice(part * sub, (part + 1) * sub)
        h_ref[at] = (x_refs[part][...].astype(F32) + acc[at].astype(BF16).astype(F32)).astype(BF16)


def project_chunk(ctx_parts, out_full, x, start, rows, place, tp_count, tile=512, sub=256):
    full_depth, width = out_full.shape
    depth = full_depth // tp_count
    n_x = rows // sub
    first = start // sub
    whole = lambda part: pl.BlockSpec(part.shape, lambda j: (0,) * part.ndim, pipeline_mode=pl.Buffered(1))
    return pl.pallas_call(
        functools.partial(project_kernel, tp_count=tp_count, n_in=len(ctx_parts), n_x=n_x),
        grid=(width // tile,),
        in_specs=[pl.BlockSpec(memory_space=pltpu.SMEM)] + [whole(p) for p in ctx_parts] + [
            pl.BlockSpec((full_depth, tile), lambda j: (0, j)),
        ] + [pl.BlockSpec((sub, tile), lambda j, r=r: (first + r, j)) for r in range(n_x)],
        out_specs=pl.BlockSpec((rows, tile), lambda j: (0, j)),
        out_shape=jax.ShapeDtypeStruct((rows, width), BF16),
        scratch_shapes=[pltpu.VMEM((tp_count, rows, depth), BF16)],
        compiler_params=pltpu.CompilerParams(vmem_limit_bytes=40 * 1024 * 1024),
        cost_estimate=pl.CostEstimate(flops=2 * rows * full_depth * width, bytes_accessed=2 * full_depth * width, transcendentals=0),
        name="project",
    )(place, *ctx_parts, out_full, *([x] * n_x))


def mlp_kernel(place_ref, h_ref, gain_ref, wg_ref, wu_ref, wd_ref, *refs, tp_count, extra):
    refs = list(refs)
    extra_ref = refs.pop(0) if extra else None
    m_ref = refs.pop()
    step = pl.program_id(0)
    rows, _ = h_ref.shape
    block = rows // tp_count
    me = place_ref[0]

    def norm(h):
        h32 = h.astype(F32)
        inv_rms = lax.rsqrt(jnp.mean(h32 * h32, axis=-1, keepdims=True) + NORM_EPS)
        return (h32 * inv_rms * gain_ref[...].astype(F32)).astype(BF16)

    @pl.when(step == 0)
    def _():
        @pl.loop(0, tp_count)
        def _(dist):
            source = lax.rem(me + dist, tp_count) * block
            m_ref[pl.ds(pl.multiple_of(dist * block, block), block), :] = norm(h_ref[pl.ds(pl.multiple_of(source, block), block), :])

        if extra:
            m_ref[rows:, :] = norm(extra_ref[...])

    gate_act = dot32(m_ref[...], wg_ref[...]).astype(BF16).astype(F32)
    up_proj = dot32(m_ref[...], wu_ref[...]).astype(BF16).astype(F32)
    swi_act = (jax.nn.silu(gate_act) * up_proj).astype(BF16)

    @pl.when(step == 0)
    def _():
        part = dot32(swi_act, wd_ref[...])
        at = 0
        for ref in refs:
            ref[...] = part[at:at + ref.shape[0]]
            at += ref.shape[0]

    @pl.when(step > 0)
    def _():
        part = dot32(swi_act, wd_ref[...])
        at = 0
        for ref in refs:
            ref[...] += part[at:at + ref.shape[0]]
            at += ref.shape[0]


def mlp_chunk(hidden, gain, gate_mat, up_mat, down_mat, place, tp_count, extra=None, tile=512):
    rows, width = hidden.shape
    ff = gate_mat.shape[1]
    block = rows // tp_count
    sizes = [block, block, block // 2, block // 2, block]
    total = rows
    operands = [place, hidden, gain, gate_mat, up_mat, down_mat]
    once = lambda shape: pl.BlockSpec(shape, lambda f: (0, 0), pipeline_mode=pl.Buffered(1))
    in_specs = [
        pl.BlockSpec(memory_space=pltpu.SMEM),
        once((rows, width)),
        once((1, width)),
        pl.BlockSpec((width, tile), lambda f: (0, f)),
        pl.BlockSpec((width, tile), lambda f: (0, f)),
        pl.BlockSpec((tile, width), lambda f: (f, 0)),
    ]
    if extra is not None:
        sizes.append(extra.shape[0])
        total += extra.shape[0]
        operands.append(extra)
        in_specs.append(once(extra.shape))
    return pl.pallas_call(
        functools.partial(mlp_kernel, tp_count=tp_count, extra=extra is not None),
        grid=(ff // tile,),
        in_specs=in_specs,
        out_specs=[once((size, width)) for size in sizes],
        out_shape=[jax.ShapeDtypeStruct((size, width), F32) for size in sizes],
        scratch_shapes=[pltpu.VMEM((total, width), BF16)],
        compiler_params=pltpu.CompilerParams(vmem_limit_bytes=60 * 1024 * 1024),
        cost_estimate=pl.CostEstimate(flops=6 * rows * width * ff, bytes_accessed=6 * width * ff, transcendentals=rows * ff),
        name="mlp",
    )(*operands)


def after(value, *deps):
    return lax.optimization_barrier((value,) + deps)[0]


def make_ring(tp_count):
    up = [(i, (i + 1) % tp_count) for i in range(tp_count)]
    down = [((i + 1) % tp_count, i) for i in range(tp_count)]
    return (lambda x: lax.ppermute(x, 'tp', up)), (lambda x: lax.ppermute(x, 'tp', down))


def ring_gather(block, tp_count):
    send_up, send_down = make_ring(tp_count)
    half = block.shape[0] // 2
    prev = send_up(block)
    succ = send_down(block)
    far_a = send_up(prev[:half])
    far_b = send_down(succ[half:])
    return [block, succ, far_a, far_b, prev]


def scatter_first(parts, tp_count):
    send_up, send_down = make_ring(tp_count)
    from_prev = send_up(parts[2])
    from_succ = send_down(parts[3])
    return from_prev, from_succ


def scatter_add(parts, first):
    from_prev, from_succ = first
    succ, prev = parts[1], parts[4]
    half = from_prev.shape[0]
    up_block = lax.dynamic_update_slice(succ, succ[:half] + from_prev, (0, 0))
    down_block = lax.dynamic_update_slice(prev, prev[half:] + from_succ, (half, 0))
    return up_block, down_block


def scatter_last(own, blocks, tp_count):
    send_up, send_down = make_ring(tp_count)
    from_prev = send_up(blocks[0])
    from_succ = send_down(blocks[1])
    return own + (from_prev + from_succ)


def small_sum(partial, tp_count):
    send_up, send_down = make_ring(tp_count)
    far = lax.ppermute(partial, 'tp', [(i, (i + 2) % tp_count) for i in range(tp_count)])
    prev = send_up(partial)
    succ = send_down(partial)
    return (partial + far) + (prev + succ)


def hand_off(pack, tp_count, node_count, tp_index):
    kv_local = pack.shape[0]
    spread = tp_count // kv_local
    got = []
    for step in range(kv_local):
        head = (tp_index // spread + step) % kv_local
        piece = lax.dynamic_index_in_dim(pack, head, axis=0, keepdims=False)
        pairs = []
        for node in range(node_count):
            for src in range(tp_count):
                h = (src // spread + step) % kv_local
                dst = (src % spread) * kv_local + h
                pairs.append((src * node_count + node, dst * node_count + (node + node_count // 2) % node_count))
        got.append(lax.ppermute(piece, ('tp', 'node'), pairs))
    first = jnp.stack([got[0], got[1]], axis=2)
    second = jnp.stack([got[1], got[0]], axis=2)
    both = jnp.where(tp_index % kv_local == 0, first, second)
    return both[0][None, None], both[1][None, None]


def write_cache(old, new, write_mask):
    return jnp.where(write_mask[:, :, :, None, None], new[:, :, None], old)


def decode_attention(q_rot, k_rot, v_new, k_old, v_old, write_mask, seen_mask):
    k_upd = write_cache(k_old, k_rot, write_mask)
    v_upd = write_cache(v_old, v_new, write_mask)
    scores = jnp.einsum('nbkgd,nbtkd->nbkgt', q_rot, k_upd, preferred_element_type=F32) * (q_rot.shape[-1] ** -0.5)
    scores = jnp.where(seen_mask[:, :, None, None, :], scores, -1e30)
    probs_bf = jax.nn.softmax(scores, axis=-1).astype(BF16)
    return jnp.einsum('nbkgt,nbtkd->nbkgd', probs_bf, v_upd, preferred_element_type=F32).astype(BF16)


def decode_attend(tokens, c_len, k_cache, v_cache, attn_gain, qkv_dec, out_dec, tp_count):
    group_size = qkv_dec.shape[2] - 2
    cos_tab, sin_tab = rope_tables(c_len, qkv_dec.shape[-1])
    cache_pos = jnp.arange(k_cache.shape[2])
    write_mask = cache_pos[None, None, :] == c_len[:, :, None]
    seen_mask = cache_pos[None, None, :] <= c_len[:, :, None]
    normed = rms_norm(tokens, attn_gain)
    qkv_all = jnp.einsum('nse,ekcd->nskcd', normed, qkv_dec, preferred_element_type=F32).astype(BF16)
    q_rot = apply_rope(qkv_all[:, :, :, :group_size], cos_tab[:, :, None, None, :], sin_tab[:, :, None, None, :])
    k_rot = apply_rope(qkv_all[:, :, :, group_size], cos_tab[:, :, None, :], sin_tab[:, :, None, :])
    v_new = qkv_all[:, :, :, group_size + 1]
    context = decode_attention(q_rot, k_rot, v_new, k_cache, v_cache, write_mask, seen_mask)
    attn_part = jnp.einsum('nskgd,kgde->nse', context, out_dec, preferred_element_type=F32)
    hidden = residual_add(tokens, small_sum(attn_part, tp_count).astype(BF16))
    return hidden, k_rot, v_new, write_mask


def solution(mesh):
    node_count = mesh.shape['node']
    tp_count = mesh.shape['tp']
    row_spec = P(('pair', 'node'), None, None)
    len_spec = P(('pair', 'node'))
    clen_spec = P(('pair', 'node'), None)
    cache_spec = P(None, ('pair', 'node'), None, None, 'tp', None)
    prompt_kv_spec = P(None, ('pair', 'node'), None, 'tp', None)
    gain_spec = P(None, None)
    qkv_spec = P(None, None, 'tp', None, None)
    out_spec = P(None, 'tp', None, None, None)
    col_spec = P(None, None, 'tp')
    down_spec = P(None, 'tp', None)

    def local_fn(prompt, s_len, tokens, c_len, k_cache, v_cache, attn_norm, mlp_norm, w_qkv_pre, w_out_pre, w_qkv_dec, w_out_dec, w_gate, w_up, w_down):
        tp_index = lax.axis_index('tp')
        node_index = lax.axis_index('node')
        width = prompt.shape[-1]
        seq_len = prompt.shape[1]
        kv_local, per_kv, head_dim = w_qkv_pre.shape[2:]
        group_size = per_kv - 2
        gate_mat, up_mat, down_mat = w_gate[0], w_up[0], w_down[0]

        out_local = w_out_pre[0].reshape(kv_local * group_size * head_dim, width)
        slice_rows = out_local.shape[0] // node_count
        out_slice = lax.dynamic_slice_in_dim(out_local, node_index * slice_rows, slice_rows, axis=0)
        out_full = lax.all_gather(out_slice, ('tp', 'node'), axis=0, tiled=True)

        x = prompt[0]
        qkv = dot32(rms_norm(x, attn_norm[0]), w_qkv_pre[0].reshape(width, kv_local * per_kv * head_dim)).astype(BF16)
        cos_tab, sin_tab = rope_tables(jnp.arange(seq_len), head_dim)
        cos_full = jnp.concatenate([cos_tab, cos_tab], axis=-1)
        sin_full = jnp.concatenate([-sin_tab, sin_tab], axis=-1)
        k_rot, pack = kv_prep(qkv, s_len, cos_full, sin_full, kv_local, group_size, head_dim)

        place = tp_index.astype(jnp.int32)[None]
        edges = chunk_edges(seq_len)
        spans = list(zip(edges[:-1], edges[1:]))
        contexts = []
        for start, stop in spans:
            lengths = after(s_len, contexts[-1]) if contexts else s_len
            contexts.append(attend_chunk(qkv, k_rot, cos_full, sin_full, lengths, start, stop - start, kv_local, group_size, head_dim))
        ctx_parts = [ring_gather(contexts[0], tp_count)]
        ctx_parts += [[lax.all_gather(context, 'tp', axis=0)] for context in contexts[1:]]
        partials, blocks, finals, hiddens, firsts = [], [], [], [], []
        tok_part = None

        def finish(c):
            summed = scatter_last(partials[c][0], blocks[c], tp_count)
            own_rows = summed.shape[0]
            own_hidden = lax.dynamic_slice_in_dim(hiddens[c], tp_index * own_rows, own_rows, axis=0)
            finals.append(residual_add(own_hidden, summed.astype(BF16)))

        for chunk, (start, stop) in enumerate(spans):
            deps = []
            if chunk >= 2:
                finish(chunk - 2)
                deps.append(finals[chunk - 2])
            if chunk >= 1:
                deps.append(partials[chunk - 1][0])
            parts = ctx_parts[chunk]
            if deps:
                parts = list(lax.optimization_barrier(tuple(parts) + tuple(deps))[:len(parts)])
            hidden = project_chunk(parts, out_full, x, start, stop - start, place, tp_count)
            if chunk >= 1:
                blocks.append(scatter_add(partials[chunk - 1], firsts[chunk - 1]))
                hidden = after(hidden, *blocks[chunk - 1])
            hiddens.append(hidden)
            extra = None
            if chunk == 2:
                held = after(tokens, partials[0][0])
                tok_hidden, k_row, v_row, write_mask = decode_attend(held, c_len, k_cache[0], v_cache[0], attn_norm[0], w_qkv_dec[0], w_out_dec[0], tp_count)
                extra = tok_hidden[0]
            partial = mlp_chunk(hidden, mlp_norm, gate_mat, up_mat, down_mat, place, tp_count, extra)
            partials.append(partial)
            if chunk == 2:
                tok_part = partial[5]
            firsts.append(scatter_first(partial, tp_count))
        finish(len(spans) - 2)
        blocks.append(scatter_add(partials[-1], firsts[-1]))
        finish(len(spans) - 1)
        out = jnp.zeros((seq_len, width), BF16)
        for final, (start, stop) in zip(finals, spans):
            out = lax.dynamic_update_slice(out, lax.all_gather(final, 'tp', axis=0, tiled=True), (start, 0))

        k_prompt, v_prompt = hand_off(after(pack, partials[0][0]), tp_count, node_count, tp_index)
        tok_sum = small_sum(tok_part[None], tp_count)
        tok_out = residual_add(tok_hidden, tok_sum.astype(BF16))
        k_row, v_row = lax.optimization_barrier((k_row, v_row, partials[-1][0]))[:2]
        k_new = write_cache(k_cache[0], k_row, write_mask)[None]
        v_new = write_cache(v_cache[0], v_row, write_mask)[None]
        return out[None], tok_out, k_prompt, v_prompt, k_new, v_new

    return jax.shard_map(local_fn, mesh=mesh, in_specs=(row_spec, len_spec, row_spec, clen_spec, cache_spec, cache_spec, gain_spec, gain_spec, qkv_spec, out_spec, qkv_spec, out_spec, col_spec, col_spec, down_spec), out_specs=(row_spec, row_spec, prompt_kv_spec, prompt_kv_spec, cache_spec, cache_spec), check_vma=False)
```

```python
import functools
import math
import jax
import jax.numpy as jnp
from jax import lax
from jax.experimental import pallas as pl
from jax.experimental.pallas import tpu as pltpu
from jax.sharding import PartitionSpec as P

NORM_EPS = 1e-5
ROPE_BASE = 10000.0
CHUNK_ROWS = 512
F32 = jnp.float32
BF16 = jnp.bfloat16


def chunk_edges(seq_len):
    return list(range(0, seq_len + 1, CHUNK_ROWS))


def rope_tables(positions, head_dim):
    inv_freq = jnp.exp(jnp.arange(head_dim // 2, dtype=F32) * (-2.0 * math.log(ROPE_BASE) / head_dim))
    angles = positions.astype(F32)[..., None] * inv_freq
    return jnp.cos(angles), jnp.sin(angles)


def apply_rope(vectors, cos_tab, sin_tab):
    half_dim = vectors.shape[-1] // 2
    vec32 = vectors.astype(F32)
    first_half = vec32[..., :half_dim]
    second_half = vec32[..., half_dim:]
    return jnp.concatenate([first_half * cos_tab - second_half * sin_tab, second_half * cos_tab + first_half * sin_tab], axis=-1).astype(BF16)


def rms_norm(hidden, gain_vec):
    hidden_f = hidden.astype(F32)
    inv_rms = lax.rsqrt(jnp.mean(hidden_f * hidden_f, axis=-1, keepdims=True) + NORM_EPS)
    return (hidden_f * inv_rms * gain_vec.astype(F32)).astype(BF16)


def residual_add(hidden, delta_bf):
    return (hidden.astype(F32) + delta_bf.astype(F32)).astype(BF16)


def dot32(a, b):
    return jnp.dot(a, b, preferred_element_type=F32)


def kv_prep_kernel(slen_ref, *refs, kv_local, head_dim, rows):
    k_refs = refs[:kv_local]
    v_refs = refs[kv_local:2 * kv_local]
    cos_ref, sin_ref, k_out, pack_out = refs[2 * kv_local:]
    pos = pl.program_id(0) * rows + lax.broadcasted_iota(jnp.int32, (rows, head_dim), 0)
    keep = pos < slen_ref[0]
    for head in range(kv_local):
        k32 = k_refs[head][...].astype(F32)
        k_rot = (k32 * cos_ref[...] + pltpu.roll(k32, head_dim // 2, 1) * sin_ref[...]).astype(BF16)
        k_out[:, head * head_dim:(head + 1) * head_dim] = k_rot
        zero = jnp.zeros_like(k_rot)
        pack_out[head, 0] = jnp.where(keep, k_rot, zero)
        pack_out[head, 1] = jnp.where(keep, v_refs[head][...], zero)


def kv_prep(qkv, s_len, cos_full, sin_full, kv_local, group_size, head_dim):
    seq_len = qkv.shape[0]
    rows = 512
    per_kv = group_size + 2
    col = lambda c: pl.BlockSpec((rows, head_dim), lambda r, c=c: (r, c))
    in_specs = [pl.BlockSpec(memory_space=pltpu.SMEM)]
    in_specs += [col(h * per_kv + group_size) for h in range(kv_local)]
    in_specs += [col(h * per_kv + group_size + 1) for h in range(kv_local)]
    in_specs += [col(0), col(0)]
    return pl.pallas_call(
        functools.partial(kv_prep_kernel, kv_local=kv_local, head_dim=head_dim, rows=rows),
        grid=(seq_len // rows,),
        in_specs=in_specs,
        out_specs=[pl.BlockSpec((rows, kv_local * head_dim), lambda r: (r, 0)), pl.BlockSpec((kv_local, 2, rows, head_dim), lambda r: (0, 0, r, 0))],
        out_shape=[jax.ShapeDtypeStruct((seq_len, kv_local * head_dim), BF16), jax.ShapeDtypeStruct((kv_local, 2, seq_len, head_dim), BF16)],
        cost_estimate=pl.CostEstimate(flops=seq_len * 4096, bytes_accessed=seq_len * 3072, transcendentals=0),
        name="kv_prep",
    )(s_len, *([qkv] * (2 * kv_local)), cos_full, sin_full)


def attend_kernel(slen_ref, *refs, start, sub, n_q):
    q_refs, cos_refs, sin_refs = refs[:n_q], refs[n_q:2 * n_q], refs[2 * n_q:3 * n_q]
    k_ref, v_ref, out_ref = refs[3 * n_q:]
    head_dim = k_ref.shape[1]
    scale = (head_dim ** -0.5) * math.log2(math.e)
    dims = (((1,), (1,)), ((), ()))
    for part in range(n_q):
        q32 = q_refs[part][...].astype(F32)
        q_part = (q32 * cos_refs[part][...] + pltpu.roll(q32, head_dim // 2, 1) * sin_refs[part][...]).astype(BF16)
        base = start + part * sub
        width = base + sub
        tail = lax.dot_general(q_part, k_ref[base:width], dims, preferred_element_type=F32)
        q_pos = lax.broadcasted_iota(jnp.int32, (sub, sub), 0)
        k_pos = lax.broadcasted_iota(jnp.int32, (sub, sub), 1)
        allowed = (k_pos <= q_pos) & (k_pos + base < slen_ref[0])
        tail = jnp.where(allowed, tail, -1e30)
        top = jnp.max(tail, axis=1, keepdims=True)
        if base > 0:
            body = lax.dot_general(q_part, k_ref[:base], dims, preferred_element_type=F32)
            safe = 1536
            if base > safe:
                k_head = lax.broadcasted_iota(jnp.int32, (sub, base - safe), 1) + safe
                late = jnp.where(k_head < slen_ref[0], body[:, safe:], -1e30)
                body = jnp.concatenate([body[:, :safe], late], axis=1)
            top = jnp.maximum(top, jnp.max(body, axis=1, keepdims=True))
            p_body = jnp.exp2((body - top) * scale)
            p_tail = jnp.exp2((tail - top) * scale)
            inv = 1.0 / (jnp.sum(p_body, axis=1, keepdims=True) + jnp.sum(p_tail, axis=1, keepdims=True))
            acc = dot32((p_body * inv).astype(BF16), v_ref[:base]) + dot32((p_tail * inv).astype(BF16), v_ref[base:width])
        else:
            p_tail = jnp.exp2((tail - top) * scale)
            inv = 1.0 / jnp.sum(p_tail, axis=1, keepdims=True)
            acc = dot32((p_tail * inv).astype(BF16), v_ref[base:width])
        out_ref[part * sub:(part + 1) * sub, :] = acc.astype(BF16)


def attend_chunk(qkv, k_rot, cos_full, sin_full, s_len, start, rows, kv_local, group_size, head_dim, sub=256):
    heads = kv_local * group_size
    per_kv = group_size + 2
    width = start + rows
    n_q = rows // sub
    first = start // sub
    tabs = [pl.BlockSpec((sub, head_dim), lambda h, r=r: (first + r, 0)) for r in range(n_q)]
    return pl.pallas_call(
        functools.partial(attend_kernel, start=start, sub=sub, n_q=n_q),
        grid=(heads,),
        in_specs=[pl.BlockSpec(memory_space=pltpu.SMEM)]
        + [pl.BlockSpec((sub, head_dim), lambda h, r=r: (first + r, (h // group_size) * per_kv + h % group_size)) for r in range(n_q)]
        + tabs + tabs + [
            pl.BlockSpec((width, head_dim), lambda h: (0, h // group_size)),
            pl.BlockSpec((width, head_dim), lambda h: (0, (h // group_size) * per_kv + group_size + 1)),
        ],
        out_specs=pl.BlockSpec((rows, head_dim), lambda h: (0, h)),
        out_shape=jax.ShapeDtypeStruct((rows, heads * head_dim), BF16),
        cost_estimate=pl.CostEstimate(flops=4 * rows * width * heads * head_dim * 3, bytes_accessed=4 * rows * heads * head_dim, transcendentals=rows * width * heads),
        name="attend",
    )(s_len, *([qkv] * n_q), *([cos_full] * n_q), *([sin_full] * n_q), k_rot, qkv)


def project_kernel(place_ref, *refs, tp_count, n_in, n_x):
    ctx_refs = refs[:n_in]
    w_ref = refs[n_in]
    x_refs = refs[n_in + 1:n_in + 1 + n_x]
    h_ref, ctx_all = refs[n_in + 1 + n_x:]

    @pl.when(pl.program_id(0) == 0)
    def _():
        if n_in == 1:
            ctx_all[...] = ctx_refs[0][...]
        else:
            own, succ, far_a, far_b, prev = ctx_refs
            me = place_ref[0]
            half = far_a.shape[0]
            ctx_all[me] = own[...]
            ctx_all[lax.rem(me + 1, tp_count)] = succ[...]
            ctx_all[lax.rem(me + 2, tp_count), :half] = far_a[...]
            ctx_all[lax.rem(me + 2, tp_count), half:] = far_b[...]
            ctx_all[lax.rem(me + 3, tp_count)] = prev[...]

    depth = ctx_all.shape[2]
    acc = dot32(ctx_all[0], w_ref[:depth])
    for block in range(1, tp_count):
        acc += dot32(ctx_all[block], w_ref[block * depth:(block + 1) * depth])
    sub = x_refs[0].shape[0]
    for part in range(n_x):
        at = slice(part * sub, (part + 1) * sub)
        h_ref[at] = (x_refs[part][...].astype(F32) + acc[at].astype(BF16).astype(F32)).astype(BF16)


def project_chunk(ctx_parts, out_full, x, start, rows, place, tp_count, tile=512, sub=256):
    full_depth, width = out_full.shape
    depth = full_depth // tp_count
    n_x = rows // sub
    first = start // sub
    whole = lambda part: pl.BlockSpec(part.shape, lambda j: (0,) * part.ndim, pipeline_mode=pl.Buffered(1))
    return pl.pallas_call(
        functools.partial(project_kernel, tp_count=tp_count, n_in=len(ctx_parts), n_x=n_x),
        grid=(width // tile,),
        in_specs=[pl.BlockSpec(memory_space=pltpu.SMEM)] + [whole(p) for p in ctx_parts] + [
            pl.BlockSpec((full_depth, tile), lambda j: (0, j)),
        ] + [pl.BlockSpec((sub, tile), lambda j, r=r: (first + r, j)) for r in range(n_x)],
        out_specs=pl.BlockSpec((rows, tile), lambda j: (0, j)),
        out_shape=jax.ShapeDtypeStruct((rows, width), BF16),
        scratch_shapes=[pltpu.VMEM((tp_count, rows, depth), BF16)],
        compiler_params=pltpu.CompilerParams(vmem_limit_bytes=40 * 1024 * 1024),
        cost_estimate=pl.CostEstimate(flops=2 * rows * full_depth * width, bytes_accessed=2 * full_depth * width, transcendentals=0),
        name="project",
    )(place, *ctx_parts, out_full, *([x] * n_x))


def mlp_kernel(place_ref, h_ref, gain_ref, wg_ref, wu_ref, wd_ref, *refs, tp_count, extra):
    refs = list(refs)
    extra_ref = refs.pop(0) if extra else None
    m_ref = refs.pop()
    step = pl.program_id(0)
    rows, _ = h_ref.shape
    block = rows // tp_count
    me = place_ref[0]

    def norm(h):
        h32 = h.astype(F32)
        inv_rms = lax.rsqrt(jnp.mean(h32 * h32, axis=-1, keepdims=True) + NORM_EPS)
        return (h32 * inv_rms * gain_ref[...].astype(F32)).astype(BF16)

    @pl.when(step == 0)
    def _():
        @pl.loop(0, tp_count)
        def _(dist):
            source = lax.rem(me + dist, tp_count) * block
            m_ref[pl.ds(pl.multiple_of(dist * block, block), block), :] = norm(h_ref[pl.ds(pl.multiple_of(source, block), block), :])

        if extra:
            m_ref[rows:, :] = norm(extra_ref[...])

    gate_act = dot32(m_ref[...], wg_ref[...]).astype(BF16).astype(F32)
    up_proj = dot32(m_ref[...], wu_ref[...]).astype(BF16).astype(F32)
    swi_act = (jax.nn.silu(gate_act) * up_proj).astype(BF16)

    @pl.when(step == 0)
    def _():
        part = dot32(swi_act, wd_ref[...])
        at = 0
        for ref in refs:
            ref[...] = part[at:at + ref.shape[0]]
            at += ref.shape[0]

    @pl.when(step > 0)
    def _():
        part = dot32(swi_act, wd_ref[...])
        at = 0
        for ref in refs:
            ref[...] += part[at:at + ref.shape[0]]
            at += ref.shape[0]


def mlp_chunk(hidden, gain, gate_mat, up_mat, down_mat, place, tp_count, extra=None, tile=512):
    rows, width = hidden.shape
    ff = gate_mat.shape[1]
    block = rows // tp_count
    sizes = [block, block, block // 2, block // 2, block]
    total = rows
    operands = [place, hidden, gain, gate_mat, up_mat, down_mat]
    once = lambda shape: pl.BlockSpec(shape, lambda f: (0, 0), pipeline_mode=pl.Buffered(1))
    in_specs = [
        pl.BlockSpec(memory_space=pltpu.SMEM),
        once((rows, width)),
        once((1, width)),
        pl.BlockSpec((width, tile), lambda f: (0, f)),
        pl.BlockSpec((width, tile), lambda f: (0, f)),
        pl.BlockSpec((tile, width), lambda f: (f, 0)),
    ]
    if extra is not None:
        sizes.append(extra.shape[0])
        total += extra.shape[0]
        operands.append(extra)
        in_specs.append(once(extra.shape))
    return pl.pallas_call(
        functools.partial(mlp_kernel, tp_count=tp_count, extra=extra is not None),
        grid=(ff // tile,),
        in_specs=in_specs,
        out_specs=[once((size, width)) for size in sizes],
        out_shape=[jax.ShapeDtypeStruct((size, width), F32) for size in sizes],
        scratch_shapes=[pltpu.VMEM((total, width), BF16)],
        compiler_params=pltpu.CompilerParams(vmem_limit_bytes=60 * 1024 * 1024),
        cost_estimate=pl.CostEstimate(flops=6 * rows * width * ff, bytes_accessed=6 * width * ff, transcendentals=rows * ff),
        name="mlp",
    )(*operands)


def after(value, *deps):
    return lax.optimization_barrier((value,) + deps)[0]


def make_ring(tp_count):
    up = [(i, (i + 1) % tp_count) for i in range(tp_count)]
    down = [((i + 1) % tp_count, i) for i in range(tp_count)]
    return (lambda x: lax.ppermute(x, 'tp', up)), (lambda x: lax.ppermute(x, 'tp', down))


def ring_gather(block, tp_count):
    send_up, send_down = make_ring(tp_count)
    half = block.shape[0] // 2
    prev = send_up(block)
    succ = send_down(block)
    far_a = send_up(prev[:half])
    far_b = send_down(succ[half:])
    return [block, succ, far_a, far_b, prev]


def scatter_first(parts, tp_count):
    send_up, send_down = make_ring(tp_count)
    from_prev = send_up(parts[2])
    from_succ = send_down(parts[3])
    return from_prev, from_succ


def scatter_add(parts, first):
    from_prev, from_succ = first
    succ, prev = parts[1], parts[4]
    half = from_prev.shape[0]
    up_block = lax.dynamic_update_slice(succ, succ[:half] + from_prev, (0, 0))
    down_block = lax.dynamic_update_slice(prev, prev[half:] + from_succ, (half, 0))
    return up_block, down_block


def scatter_last(own, blocks, tp_count):
    send_up, send_down = make_ring(tp_count)
    from_prev = send_up(blocks[0])
    from_succ = send_down(blocks[1])
    return own + (from_prev + from_succ)


def small_sum(partial, tp_count):
    send_up, send_down = make_ring(tp_count)
    far = lax.ppermute(partial, 'tp', [(i, (i + 2) % tp_count) for i in range(tp_count)])
    prev = send_up(partial)
    succ = send_down(partial)
    return (partial + far) + (prev + succ)


def hand_off(pack, tp_count, node_count, tp_index):
    kv_local = pack.shape[0]
    spread = tp_count // kv_local
    got = []
    for step in range(kv_local):
        head = (tp_index // spread + step) % kv_local
        piece = lax.dynamic_index_in_dim(pack, head, axis=0, keepdims=False)
        pairs = []
        for node in range(node_count):
            for src in range(tp_count):
                h = (src // spread + step) % kv_local
                dst = (src % spread) * kv_local + h
                pairs.append((src * node_count + node, dst * node_count + (node + node_count // 2) % node_count))
        got.append(lax.ppermute(piece, ('tp', 'node'), pairs))
    first = jnp.stack([got[0], got[1]], axis=2)
    second = jnp.stack([got[1], got[0]], axis=2)
    both = jnp.where(tp_index % kv_local == 0, first, second)
    return both[0][None, None], both[1][None, None]


def write_cache(old, new, write_mask):
    return jnp.where(write_mask[:, :, :, None, None], new[:, :, None], old)


def decode_attention(q_rot, k_rot, v_new, k_old, v_old, write_mask, seen_mask):
    k_upd = write_cache(k_old, k_rot, write_mask)
    v_upd = write_cache(v_old, v_new, write_mask)
    scores = jnp.einsum('nbkgd,nbtkd->nbkgt', q_rot, k_upd, preferred_element_type=F32) * (q_rot.shape[-1] ** -0.5)
    scores = jnp.where(seen_mask[:, :, None, None, :], scores, -1e30)
    probs_bf = jax.nn.softmax(scores, axis=-1).astype(BF16)
    return jnp.einsum('nbkgt,nbtkd->nbkgd', probs_bf, v_upd, preferred_element_type=F32).astype(BF16)


def decode_attend(tokens, c_len, k_cache, v_cache, attn_gain, qkv_dec, out_dec, tp_count):
    group_size = qkv_dec.shape[2] - 2
    cos_tab, sin_tab = rope_tables(c_len, qkv_dec.shape[-1])
    cache_pos = jnp.arange(k_cache.shape[2])
    write_mask = cache_pos[None, None, :] == c_len[:, :, None]
    seen_mask = cache_pos[None, None, :] <= c_len[:, :, None]
    normed = rms_norm(tokens, attn_gain)
    qkv_all = jnp.einsum('nse,ekcd->nskcd', normed, qkv_dec, preferred_element_type=F32).astype(BF16)
    q_rot = apply_rope(qkv_all[:, :, :, :group_size], cos_tab[:, :, None, None, :], sin_tab[:, :, None, None, :])
    k_rot = apply_rope(qkv_all[:, :, :, group_size], cos_tab[:, :, None, :], sin_tab[:, :, None, :])
    v_new = qkv_all[:, :, :, group_size + 1]
    context = decode_attention(q_rot, k_rot, v_new, k_cache, v_cache, write_mask, seen_mask)
    attn_part = jnp.einsum('nskgd,kgde->nse', context, out_dec, preferred_element_type=F32)
    hidden = residual_add(tokens, small_sum(attn_part, tp_count).astype(BF16))
    return hidden, k_rot, v_new, write_mask


def solution(mesh):
    node_count = mesh.shape['node']
    tp_count = mesh.shape['tp']
    row_spec = P(('pair', 'node'), None, None)
    len_spec = P(('pair', 'node'))
    clen_spec = P(('pair', 'node'), None)
    cache_spec = P(None, ('pair', 'node'), None, None, 'tp', None)
    prompt_kv_spec = P(None, ('pair', 'node'), None, 'tp', None)
    gain_spec = P(None, None)
    qkv_spec = P(None, None, 'tp', None, None)
    out_spec = P(None, 'tp', None, None, None)
    col_spec = P(None, None, 'tp')
    down_spec = P(None, 'tp', None)

    def local_fn(prompt, s_len, tokens, c_len, k_cache, v_cache, attn_norm, mlp_norm, w_qkv_pre, w_out_pre, w_qkv_dec, w_out_dec, w_gate, w_up, w_down):
        tp_index = lax.axis_index('tp')
        node_index = lax.axis_index('node')
        width = prompt.shape[-1]
        seq_len = prompt.shape[1]
        kv_local, per_kv, head_dim = w_qkv_pre.shape[2:]
        group_size = per_kv - 2
        gate_mat, up_mat, down_mat = w_gate[0], w_up[0], w_down[0]

        out_local = w_out_pre[0].reshape(kv_local * group_size * head_dim, width)
        slice_rows = out_local.shape[0] // node_count
        out_slice = lax.dynamic_slice_in_dim(out_local, node_index * slice_rows, slice_rows, axis=0)
        out_full = lax.all_gather(out_slice, ('tp', 'node'), axis=0, tiled=True)

        x = prompt[0]
        qkv = dot32(rms_norm(x, attn_norm[0]), w_qkv_pre[0].reshape(width, kv_local * per_kv * head_dim)).astype(BF16)
        cos_tab, sin_tab = rope_tables(jnp.arange(seq_len), head_dim)
        cos_full = jnp.concatenate([cos_tab, cos_tab], axis=-1)
        sin_full = jnp.concatenate([-sin_tab, sin_tab], axis=-1)
        k_rot, pack = kv_prep(qkv, s_len, cos_full, sin_full, kv_local, group_size, head_dim)

        place = tp_index.astype(jnp.int32)[None]
        edges = chunk_edges(seq_len)
        spans = list(zip(edges[:-1], edges[1:]))
        contexts = []
        for start, stop in spans:
            lengths = after(s_len, contexts[-1]) if contexts else s_len
            contexts.append(attend_chunk(qkv, k_rot, cos_full, sin_full, lengths, start, stop - start, kv_local, group_size, head_dim))
        ctx_parts = [ring_gather(contexts[0], tp_count)]
        ctx_parts += [[lax.all_gather(context, 'tp', axis=0)] for context in contexts[1:]]
        partials, blocks, finals, hiddens, firsts = [], [], [], [], []
        tok_part = None

        def finish(c):
            summed = scatter_last(partials[c][0], blocks[c], tp_count)
            own_rows = summed.shape[0]
            own_hidden = lax.dynamic_slice_in_dim(hiddens[c], tp_index * own_rows, own_rows, axis=0)
            finals.append(residual_add(own_hidden, summed.astype(BF16)))

        for chunk, (start, stop) in enumerate(spans):
            deps = []
            if chunk >= 2:
                finish(chunk - 2)
                deps.append(finals[chunk - 2])
            if chunk >= 1:
                deps.append(partials[chunk - 1][0])
            parts = ctx_parts[chunk]
            if deps:
                parts = list(lax.optimization_barrier(tuple(parts) + tuple(deps))[:len(parts)])
            hidden = project_chunk(parts, out_full, x, start, stop - start, place, tp_count)
            if chunk >= 1:
                blocks.append(scatter_add(partials[chunk - 1], firsts[chunk - 1]))
                hidden = after(hidden, *blocks[chunk - 1])
            hiddens.append(hidden)
            extra = None
            if chunk == 2:
                held = after(tokens, partials[0][0])
                tok_hidden, k_row, v_row, write_mask = decode_attend(held, c_len, k_cache[0], v_cache[0], attn_norm[0], w_qkv_dec[0], w_out_dec[0], tp_count)
                extra = tok_hidden[0]
            partial = mlp_chunk(hidden, mlp_norm, gate_mat, up_mat, down_mat, place, tp_count, extra)
            partials.append(partial)
            if chunk == 2:
                tok_part = partial[5]
            firsts.append(scatter_first(partial, tp_count))
        finish(len(spans) - 2)
        blocks.append(scatter_add(partials[-1], firsts[-1]))
        finish(len(spans) - 1)
        out = jnp.zeros((seq_len, width), BF16)
        for final, (start, stop) in zip(finals, spans):
            out = lax.dynamic_update_slice(out, lax.all_gather(final, 'tp', axis=0, tiled=True), (start, 0))

        k_prompt, v_prompt = hand_off(after(pack, partials[0][0]), tp_count, node_count, tp_index)
        tok_sum = small_sum(tok_part[None], tp_count)
        tok_out = residual_add(tok_hidden, tok_sum.astype(BF16))
        k_row, v_row = lax.optimization_barrier((k_row, v_row, partials[-1][0]))[:2]
        k_new = write_cache(k_cache[0], k_row, write_mask)[None]
        v_new = write_cache(v_cache[0], v_row, write_mask)[None]
        return out[None], tok_out, k_prompt, v_prompt, k_new, v_new

    return jax.shard_map(local_fn, mesh=mesh, in_specs=(row_spec, len_spec, row_spec, clen_spec, cache_spec, cache_spec, gain_spec, gain_spec, qkv_spec, out_spec, qkv_spec, out_spec, col_spec, col_spec, down_spec), out_specs=(row_spec, row_spec, prompt_kv_spec, prompt_kv_spec, cache_spec, cache_spec), check_vma=False)
```
